32 devices in a mesh: wide: 8 (over z, core), narrow: 4 (over y, x).
Axes of the slice: x: 2, y: 2, z: 4, core: 2. Of those that a mesh axis runs over, the one named last changes fastest.
Arguments:
- pixel_stack: float32 [128, 64, 2048], P(('wide', 'narrow')), may hold values from -6 to 6
- quality_weight: float32 [128, 64, 2048], P(('wide', 'narrow')), may hold values from 0.2 to 1
Outputs:
- slope: float32 [64, 2048], P('wide', 'narrow')
- level: float32 [64, 2048], P('wide', 'narrow')
- anomaly: bfloat16 [128, 64, 2048], P(None, 'wide', 'narrow')
The draws below stay inside these ranges and needn't reach their ends.
All inputs are finite; a program needn't handle non-finite values.
Results may differ from the reference program's by a relative error of at most 0.001.
Values sent between devices are 32-bit elements; how exact they have to be, the bound alone decides.
No kernel may reach another device: no remote copies, remote signals or barrier semaphores. Data moves between devices by JAX's collectives and lax.ppermute only.
A program may use at most 64 MiB of HBM per device.

```python
import jax
import jax.numpy as jnp
from jax import lax

TSTEPS = 128
ROWS_DEV = 8
H = 64
W = 2048


def steps_of(own_key, dims, shards, low, largest):
    def one(position, parts):
        heights = jax.random.uniform(jax.random.fold_in(jax.random.fold_in(own_key, 6), position), (parts,), jnp.float32, low / len(shards), largest / len(shards))
        return jnp.repeat(jnp.exp(heights), dims[position] // parts).reshape((-1,) + (1,) * (len(dims) - position - 1))

    loudness = one(*shards[0])
    for cut in shards[1:]:
        loudness = loudness * one(*cut)
    return loudness


def noise(key, extent, deviation, most, cuts=(), dtype=jnp.bfloat16):
    result = deviation * jax.random.normal(key, extent, jnp.float32)
    if cuts:
        result = result * steps_of(key, extent, cuts, -0.22, 0.18)
    return jnp.clip(result, -most, most).astype(dtype)


def setup_inputs(seed: int = 0) -> dict:
    key_of = jax.random.split(jax.random.key(seed), 3)
    pixel_stack = noise(key_of[0], (TSTEPS, H, W), 1.0, 6.0, ((0, 32),), jnp.float32)
    quality_weight = jnp.clip(0.2 + 0.8 * jax.random.uniform(key_of[1], (TSTEPS, H, W), jnp.float32) ** steps_of(key_of[1], (TSTEPS, H, W), ((0, 32),), -0.2, 0.2), 0.2, 1.0)
    return {"pixel_stack": pixel_stack, "quality_weight": quality_weight}


def fit_trend(series, weight_series):
    count = series.shape[0]
    centred = ((jnp.arange(count).astype(jnp.float32) - (count - 1) / 2.0) / count).reshape(count, 1, 1)
    weighted = weight_series * series
    first = jnp.sum(weight_series, axis=0)
    second = jnp.sum(weight_series * centred, axis=0)
    third = jnp.sum(weight_series * centred * centred, axis=0)
    plain_sum = jnp.sum(weighted, axis=0)
    moment_sum = jnp.sum(weighted * centred, axis=0)
    determinant = first * third - second * second
    slope = (first * moment_sum - second * plain_sum) / determinant
    level = (third * plain_sum - second * moment_sum) / determinant
    anomaly = (series - level[None] - slope[None] * centred).astype(jnp.bfloat16)
    return slope, level, anomaly


def reference(pixel_stack, quality_weight):
    blocks = H // ROWS_DEV
    series = pixel_stack.reshape(TSTEPS, blocks, ROWS_DEV, W).transpose(1, 0, 2, 3)
    weights = quality_weight.reshape(TSTEPS, blocks, ROWS_DEV, W).transpose(1, 0, 2, 3)
    slope, level, anomaly = lax.map(lambda pair: fit_trend(pair[0], pair[1]), (series, weights))
    slope = slope.reshape(H, W)
    level = level.reshape(H, W)
    anomaly = anomaly.transpose(1, 0, 2, 3).reshape(TSTEPS, H, W)
    return slope, level, anomaly
```

```python
import jax
import jax.numpy as jnp
from jax import lax
from jax.sharding import PartitionSpec as P


def body(pixel_stack, quality_weight):
    wide_count = lax.axis_size("wide")
    narrow_count = lax.axis_size("narrow")
    wide = lax.axis_index("wide")
    narrow = lax.axis_index("narrow")
    local_steps = pixel_stack.shape[0]
    rows_tile = pixel_stack.shape[1] // wide_count
    cols_tile = pixel_stack.shape[2] // narrow_count
    count = local_steps * wide_count * narrow_count

    split = pixel_stack.reshape(local_steps, wide_count, rows_tile, narrow_count, cols_tile)
    tiles = split.transpose(1, 3, 0, 2, 4).reshape(
        wide_count * narrow_count, local_steps, rows_tile, cols_tile
    )
    series = lax.all_to_all(tiles, ("wide", "narrow"), split_axis=0, concat_axis=1, tiled=True)
    series = series.reshape(count, rows_tile, cols_tile)

    first_step = (wide * narrow_count + narrow) * local_steps
    steps = (first_step + jnp.arange(local_steps)).astype(jnp.float32)
    centred = ((steps - (count - 1) / 2.0) / count).reshape(local_steps, 1, 1)
    weighted = quality_weight * pixel_stack
    sums = jnp.stack([
        jnp.sum(quality_weight, axis=0),
        jnp.sum(quality_weight * centred, axis=0),
        jnp.sum(quality_weight * centred * centred, axis=0),
        jnp.sum(weighted, axis=0),
        jnp.sum(weighted * centred, axis=0),
    ])
    sums = sums.reshape(5, wide_count, rows_tile, narrow_count, cols_tile).transpose(1, 3, 0, 2, 4)

    def halve(sums, axis, bit):
        dim = 0 if axis == "wide" else 1
        size = lax.axis_size(axis)
        index = lax.axis_index(axis)
        return None

    def exchange(part, axis, bit):
        size = lax.axis_size(axis)
        return lax.ppermute(part, axis, [(i, i ^ bit) for i in range(size)])

    shape = sums.shape
    half = wide_count // 2
    s = sums.reshape(half, 2, narrow_count, 5, rows_tile, cols_tile)
    mine = wide % 2
    keep = lax.dynamic_index_in_dim(s, mine, 1, keepdims=False)
    send = lax.dynamic_index_in_dim(s, 1 - mine, 1, keepdims=False)
    s = keep + exchange(send, "wide", 1)
    total = lax.dynamic_index_in_dim(s, narrow, 1, keepdims=False)
    for d in range(1, narrow_count):
        part = lax.dynamic_index_in_dim(s, narrow ^ d, 1, keepdims=False)
        total = total + exchange(part, "narrow", d)
    s = total
    bit = 1
    while bit < half:
        n = s.shape[0]
        s = s.reshape(n // 2, 2, 5, rows_tile, cols_tile)
        mine = (wide // (2 * bit)) % 2
        keep = lax.dynamic_index_in_dim(s, mine, 1, keepdims=False)
        send = lax.dynamic_index_in_dim(s, 1 - mine, 1, keepdims=False)
        s = keep + exchange(send, "wide", 2 * bit)
        bit *= 2
    first, second, third, plain_sum, moment_sum = [s[0, i] for i in range(5)]
    determinant = first * third - second * second
    slope = (first * moment_sum - second * plain_sum) / determinant
    level = (third * plain_sum - second * moment_sum) / determinant
    every = ((jnp.arange(count).astype(jnp.float32) - (count - 1) / 2.0) / count).reshape(count, 1, 1)
    anomaly = (series - level[None] - slope[None] * every).astype(jnp.bfloat16)
    return slope, level, anomaly


def solution(mesh):
    return jax.shard_map(
        body,
        mesh=mesh,
        in_specs=(P(("wide", "narrow"), None, None), P(("wide", "narrow"), None, None)),
        out_specs=(P("wide", "narrow"), P("wide", "narrow"), P(None, "wide", "narrow")),
        check_vma=False,
    )
```
